32 devices in a mesh: dp: 8 (over z, core), tp: 4 (over y, x).
Axes of the slice: x: 2, y: 2, z: 4, core: 2. Of those that a mesh axis runs over, the one named last changes fastest.
Arguments:
- master: float32 [4096, 10240], P(('dp', 'tp')), may hold values from -0.09375 to 0.09375
- grad: float32 [4096, 10240], P(('dp', 'tp')), may hold values from -0.006 to 0.006
- exp_avg: float32 [4096, 10240], P(('dp', 'tp')), may hold values from -0.006 to 0.006
- exp_avg_sq: float32 [4096, 10240], P(('dp', 'tp')), may hold values from 1e-08 to 1e-05
Outputs:
- new_master: float32 [4096, 10240], P(('dp', 'tp'))
- new_avg: float32 [4096, 10240], P(('dp', 'tp'))
- new_avg_sq: float32 [4096, 10240], P(('dp', 'tp'))
- engine_qkv: bfloat16 [4096, 10240], P(None, 'tp')
The draws below stay inside these ranges and needn't reach their ends.
All inputs are finite; a program needn't handle non-finite values.
Results may differ from the reference program's by a relative error of at most 0.001.
Values may be sent and summed in bfloat16 or wider, within the bound.
No kernel may reach another device: no remote copies, remote signals or barrier semaphores. Data moves between devices by JAX's collectives and lax.ppermute only.
A program may use at most 128 MiB of HBM per device.

```python
import math
import jax
import jax.numpy as jnp

QH = 64
KVH = 8
HS = 128
D_WIN = 4096
QKVW = 10240
N_TP = 4


def level_of(own_key, dims, pieces, smallest, top_value):
    def one(position, shards_of):
        heights = jax.random.uniform(jax.random.fold_in(jax.random.fold_in(own_key, 6), position), (shards_of,), jnp.float32, smallest / len(pieces), top_value / len(pieces))
        return jnp.repeat(jnp.exp(heights), dims[position] // shards_of).reshape((-1,) + (1,) * (len(dims) - position - 1))

    gain = one(*pieces[0])
    for cut in pieces[1:]:
        gain = gain * one(*cut)
    return gain


def scatter_about(rng, extent, width, most, shards=(), dtype=jnp.bfloat16):
    array = jax.random.normal(rng, extent, jnp.float32) * width
    if len(shards) > 0:
        array = level_of(rng, extent, shards, -0.22, 0.18) * array
    return jnp.clip(array, min=-most, max=most).astype(dtype)


def setup_inputs(seed: int = 0) -> dict:
    arg_keys = jax.random.split(jax.random.key(seed), 5)
    return {
        "master": scatter_about(arg_keys[0], (D_WIN, QKVW), D_WIN ** -0.5, 0.09375, ((0, 32),), jnp.float32),
        "grad": scatter_about(arg_keys[1], (D_WIN, QKVW), 0.001, 0.006, ((0, 32),), jnp.float32),
        "exp_avg": scatter_about(arg_keys[2], (D_WIN, QKVW), 0.001, 0.006, ((0, 32),), jnp.float32),
        "exp_avg_sq": jnp.clip(jnp.exp(math.log(9.999999747378752e-06) - 6.9077553 * jax.random.uniform(arg_keys[3], (D_WIN, QKVW), jnp.float32) ** level_of(arg_keys[3], (D_WIN, QKVW), ((0, 32),), -0.2, 0.2)), 9.99999993922529e-09, 9.999999747378752e-06),
    }


def joined_slices(weights, tp_count):
    rows = weights.shape[0]
    query = weights[:, :QH * HS].reshape(rows, tp_count, QH // tp_count * HS)
    keys = weights[:, QH * HS:(QH + KVH) * HS].reshape(rows, tp_count, KVH // tp_count * HS)
    values = weights[:, (QH + KVH) * HS:].reshape(rows, tp_count, KVH // tp_count * HS)
    return jnp.concatenate([query, keys, values], axis=2).reshape(rows, -1)

def reference(master, grad, exp_avg, exp_avg_sq):
    corr_one = 1.0 - 0.9 ** 10
    corr_two = 1.0 - 0.999 ** 10
    new_avg = 0.9 * exp_avg + 0.1 * grad
    new_avg_sq = 0.999 * exp_avg_sq + 0.001 * grad * grad
    update = new_avg / corr_one / (jnp.sqrt(new_avg_sq / corr_two) + 1e-08)
    new_master = master - 0.001 * (update + 0.1 * master)
    engine_qkv = joined_slices(new_master, N_TP).astype(jnp.bfloat16)
    return (new_master, new_avg, new_avg_sq, engine_qkv)
```

```python
import functools

import jax
import jax.numpy as jnp
from jax import lax
from jax.experimental import pallas as pl
from jax.experimental.pallas import tpu as pltpu
from jax.sharding import PartitionSpec as P

QH = 64
KVH = 8
HS = 128
CORES = 2


def step_kernel(which, master, grad, avg, sq, *refs):
    new_master, new_avg, new_sq, piece = refs[-4:]
    corr_one = 1.0 - 0.9**10
    corr_two = 1.0 - 0.999**10
    g = grad[...]
    m = 0.9 * avg[...] + 0.1 * g
    v = 0.999 * sq[...] + 0.001 * g * g
    update = m / corr_one / (jnp.sqrt(v / corr_two) + 1e-08)
    w = master[...]
    w = w - 0.001 * (update + 0.1 * w)
    new_avg[...] = m
    new_sq[...] = v
    new_master[...] = w
    piece[...] = w.astype(jnp.bfloat16)


def step_slice(which, args, filled, tp_count):
    rows, cols = args[0].shape
    width = KVH // tp_count * HS
    per_query = QH // KVH
    steps = per_query + 2

    def column(j, s):
        query = s[0] * per_query + j
        other = (per_query + j - per_query) * tp_count + s[0]
        return (0, jnp.where(j < per_query, query, other))

    wide = pl.BlockSpec((rows, width), column)
    in_specs = [wide] * 4 + [pl.BlockSpec(memory_space=pl.ANY)] * len(filled)
    out_shape = [jax.ShapeDtypeStruct((rows, cols), jnp.float32)] * 3
    out_shape.append(jax.ShapeDtypeStruct((rows, steps * width), jnp.bfloat16))
    return pl.pallas_call(
        step_kernel,
        grid_spec=pltpu.PrefetchScalarGridSpec(
            num_scalar_prefetch=1,
            grid=(steps,),
            in_specs=in_specs,
            out_specs=[wide] * 3 + [pl.BlockSpec((rows, width), lambda j, s: (0, j))],
        ),
        out_shape=out_shape,
        input_output_aliases={5 + i: i for i in range(len(filled))},
    )(which.reshape(1), *args, *filled)


def place_kernel(count, where, *refs):
    pieces = refs[:count]
    out, sems = refs[-2:]
    rows = pieces[0].shape[0]

    def copy(i):
        start = pl.multiple_of(jnp.maximum(where[i], 0) * rows, rows)
        return pltpu.make_async_copy(pieces[i], out.at[pl.ds(start, rows), :], sems.at[i])

    for i in range(count):
        pl.when(where[i] >= 0)(lambda i=i: copy(i).start())
    for i in range(count):
        pl.when(where[i] >= 0)(lambda i=i: copy(i).wait())


def place(out, shape, pieces, where):
    count = len(pieces)
    filled = [] if out is None else [out]
    return pl.pallas_call(
        functools.partial(place_kernel, count),
        in_specs=[pl.BlockSpec(memory_space=pltpu.SMEM)]
        + [pl.BlockSpec(memory_space=pl.ANY)] * (count + len(filled)),
        out_specs=pl.BlockSpec(memory_space=pl.ANY),
        out_shape=jax.ShapeDtypeStruct(shape, jnp.bfloat16),
        scratch_shapes=[pltpu.SemaphoreType.DMA((count,))],
        input_output_aliases={1 + count: 0} if filled else {},
    )(jnp.stack(where).astype(jnp.int32), *pieces, *filled)


def body(master, grad, exp_avg, exp_avg_sq):
    dp_count = lax.axis_size("dp")
    tp_count = lax.axis_size("tp")
    cores = CORES if dp_count % CORES == 0 else 1
    chips = dp_count // cores
    dp = lax.axis_index("dp")
    tp = lax.axis_index("tp")
    z = dp // cores
    core = dp % cores

    args = (master, grad, exp_avg, exp_avg_sq)
    filled = []
    sends = []
    for k in range(tp_count):
        *filled, piece = step_slice((tp ^ k).astype(jnp.int32), args, filled, tp_count)
        sends.append(piece)
    own = [sends[0]]
    for k in range(1, tp_count):
        own.append(lax.ppermute(sends[k], "tp", [(i, i ^ k) for i in range(tp_count)]))

    def along(value, step, low, high):
        pairs = [(c * cores + i, (c + step) * cores + i) for c in range(low, high) for i in range(cores)]
        return lax.ppermute(value, "dp", pairs)

    def sibling(value, low, high):
        pairs = [(c * cores + i, c * cores + 1 - i) for c in range(low, high) for i in range(cores)]
        return lax.ppermute(value, "dp", pairs)

    shape = (dp_count * tp_count * master.shape[0], own[0].shape[1])
    arrivals = []

    def arrive(value, k, chip, low, high):
        valid = (z >= low) & (z < high)
        block = (chip * cores + core) * tp_count + (tp ^ k)
        pieces, where = [value], [jnp.where(valid, block, -1)]
        if cores == 2:
            pieces.append(sibling(value, low, high))
            block = (chip * cores + 1 - core) * tp_count + (tp ^ k)
            where.append(jnp.where(valid, block, -1))
        arrivals.append((pieces, where))

    for k in range(tp_count):
        arrive(own[k], k, z, 0, chips)
    up, down = list(own), list(own)
    for r in range(1, chips):
        for k in range(tp_count):
            up[k] = along(up[k], 1, r - 1, chips - 1)
            down[k] = along(down[k], -1, 1, chips - r + 1)
            arrive(up[k], k, z - r, r, chips)
            arrive(down[k], k, z + r, 0, chips - r)

    out = None
    for pieces, where in arrivals:
        out = place(out, shape, pieces, where)
    return (*filled, out)


def solution(mesh):
    rows = P(("dp", "tp"), None)
    return jax.shard_map(
        body, mesh=mesh, in_specs=(rows,) * 4, out_specs=(rows, rows, rows, P(None, "tp")), check_vma=False
    )
```

```python
import jax
import jax.numpy as jnp
from jax import lax
from jax.experimental import pallas as pl
from jax.experimental.pallas import tpu as pltpu
from jax.sharding import PartitionSpec as P

QH = 64
KVH = 8
HS = 128


def step_kernel(which, master, grad, avg, sq, *refs):
    new_master, new_avg, new_sq, piece = refs[-4:]
    corr_one = 1.0 - 0.9**10
    corr_two = 1.0 - 0.999**10
    g = grad[...]
    m = 0.9 * avg[...] + 0.1 * g
    v = 0.999 * sq[...] + 0.001 * g * g
    update = m / corr_one / (jnp.sqrt(v / corr_two) + 1e-08)
    w = master[...]
    w = w - 0.001 * (update + 0.1 * w)
    new_avg[...] = m
    new_sq[...] = v
    new_master[...] = w
    piece[...] = w.astype(jnp.bfloat16)


def step_slice(which, args, filled, tp_count):
    rows, cols = args[0].shape
    width = KVH // tp_count * HS
    per_query = QH // KVH
    steps = per_query + 2

    def column(j, s):
        query = s[0] * per_query + j
        other = (per_query + j - per_query) * tp_count + s[0]
        return (0, jnp.where(j < per_query, query, other))

    wide = pl.BlockSpec((rows, width), column)
    in_specs = [wide] * 4 + [pl.BlockSpec(memory_space=pl.ANY)] * len(filled)
    out_shape = [jax.ShapeDtypeStruct((rows, cols), jnp.float32)] * 3
    out_shape.append(jax.ShapeDtypeStruct((rows, steps * width), jnp.bfloat16))
    return pl.pallas_call(
        step_kernel,
        grid_spec=pltpu.PrefetchScalarGridSpec(
            num_scalar_prefetch=1,
            grid=(steps,),
            in_specs=in_specs,
            out_specs=[wide] * 3 + [pl.BlockSpec((rows, width), lambda j, s: (0, j))],
        ),
        out_shape=out_shape,
        input_output_aliases={5 + i: i for i in range(len(filled))},
    )(which.reshape(1), *args, *filled)


def place_kernel(source, piece, *refs):
    refs[-1][...] = piece[...]


def place(out, gathered, source, tp_count, rows):
    width = gathered.shape[1]
    count = gathered.shape[0] // rows
    filled = [] if out is None else [out]
    return pl.pallas_call(
        place_kernel,
        grid_spec=pltpu.PrefetchScalarGridSpec(
            num_scalar_prefetch=1,
            grid=(count,),
            in_specs=[pl.BlockSpec((rows, width), lambda j, s: (j, 0))]
            + [pl.BlockSpec(memory_space=pl.ANY)] * len(filled),
            out_specs=pl.BlockSpec((rows, width), lambda j, s: (j * tp_count + s[0], 0)),
        ),
        out_shape=jax.ShapeDtypeStruct((gathered.shape[0] * tp_count, width), gathered.dtype),
        input_output_aliases={2: 0} if filled else {},
    )(source.reshape(1), gathered, *filled)


def body(master, grad, exp_avg, exp_avg_sq):
    tp_count = lax.axis_size("tp")
    tp = lax.axis_index("tp").astype(jnp.int32)
    rows = master.shape[0]
    args = (master, grad, exp_avg, exp_avg_sq)
    filled = []
    gathers = []
    for k in range(tp_count):
        *filled, piece = step_slice(tp ^ k, args, filled, tp_count)
        if k > 0:
            piece = lax.ppermute(piece, "tp", [(i, i ^ k) for i in range(tp_count)])
        gathers.append(lax.all_gather(piece, "dp", axis=0, tiled=True))
    out = None
    for k, gathered in enumerate(gathers):
        out = place(out, gathered, tp ^ k, tp_count, rows)
    return (*filled, out)


def solution(mesh):
    rows = P(("dp", "tp"), None)
    return jax.shard_map(
        body, mesh=mesh, in_specs=(rows,) * 4, out_specs=(rows, rows, rows, P(None, "tp")), check_vma=False
    )
```

```python
import jax
import jax.numpy as jnp
from jax import lax
from jax.experimental import pallas as pl
from jax.experimental.pallas import tpu as pltpu
from jax.sharding import PartitionSpec as P

QH = 64
KVH = 8
HS = 128


def step(master, grad, exp_avg, exp_avg_sq):
    corr_one = 1.0 - 0.9**10
    corr_two = 1.0 - 0.999**10
    new_avg = 0.9 * exp_avg + 0.1 * grad
    new_avg_sq = 0.999 * exp_avg_sq + 0.001 * grad * grad
    update = new_avg / corr_one / (jnp.sqrt(new_avg_sq / corr_two) + 1e-08)
    new_master = master - 0.001 * (update + 0.1 * master)
    return new_master, new_avg, new_avg_sq


def slice_kernel(which, master, grad, avg, sq, piece):
    piece[...] = step(master[...], grad[...], avg[...], sq[...])[0].astype(jnp.bfloat16)


def step_slice(which, args, tp_count):
    rows = args[0].shape[0]
    width = KVH // tp_count * HS
    per_query = QH // KVH
    steps = per_query + 2

    def column(j, s):
        return (0, jnp.where(j < per_query, s[0] * per_query + j, j * tp_count + s[0]))

    return pl.pallas_call(
        slice_kernel,
        grid_spec=pltpu.PrefetchScalarGridSpec(
            num_scalar_prefetch=1,
            grid=(steps,),
            in_specs=[pl.BlockSpec((rows, width), column)] * 4,
            out_specs=pl.BlockSpec((rows, width), lambda j, s: (0, j)),
        ),
        out_shape=jax.ShapeDtypeStruct((rows, steps * width), jnp.bfloat16),
    )(which.reshape(1), *args)


def joined_slices(weights, tp_count):
    rows = weights.shape[0]
    query = weights[:, : QH * HS].reshape(rows, tp_count, QH // tp_count * HS)
    keys = weights[:, QH * HS : (QH + KVH) * HS].reshape(rows, tp_count, KVH // tp_count * HS)
    values = weights[:, (QH + KVH) * HS :].reshape(rows, tp_count, KVH // tp_count * HS)
    return jnp.concatenate([query, keys, values], axis=2)


def place(out, gathered, tp, first, last, tp_count, rows):
    width = gathered.shape[1]
    kinds = last - first
    count = gathered.shape[0] // rows
    filled = [] if out is None else [out]

    def kernel(tp_ref, src, *refs):
        dst, held, sem_in, sem_out = refs[-4:]

        def load(i):
            return pltpu.make_async_copy(src.at[pl.ds(i * rows, rows), :], held.at[i], sem_in.at[i])

        def store(i):
            block = (i // kinds) * tp_count + (tp_ref[0] ^ (first + i % kinds))
            start = pl.multiple_of(block * rows, rows)
            return pltpu.make_async_copy(held.at[i], dst.at[pl.ds(start, rows), :], sem_out.at[i])

        for i in range(count):
            load(i).start()
        for i in range(count):
            load(i).wait()
            store(i).start()
        for i in range(count):
            store(i).wait()

    total = gathered.shape[0] // kinds * tp_count
    return pl.pallas_call(
        kernel,
        in_specs=[pl.BlockSpec(memory_space=pltpu.SMEM)]
        + [pl.BlockSpec(memory_space=pl.ANY)] * (1 + len(filled)),
        out_specs=pl.BlockSpec(memory_space=pl.ANY),
        out_shape=jax.ShapeDtypeStruct((total, width), gathered.dtype),
        scratch_shapes=[
            pltpu.VMEM((count, rows, width), gathered.dtype),
            pltpu.SemaphoreType.DMA((count,)),
            pltpu.SemaphoreType.DMA((count,)),
        ],
        input_output_aliases={2: 0} if filled else {},
    )(tp.reshape(1), gathered, *filled)


def body(master, grad, exp_avg, exp_avg_sq):
    tp_count = lax.axis_size("tp")
    tp = lax.axis_index("tp").astype(jnp.int32)
    rows = master.shape[0]
    args = (master, grad, exp_avg, exp_avg_sq)
    own = step_slice(tp, args, tp_count)
    own_gathered = lax.all_gather(own, "dp", axis=0, tiled=True)
    *args, own = lax.optimization_barrier((*args, own))
    new_master, new_avg, new_avg_sq = step(*args)
    ordered = joined_slices(new_master.astype(jnp.bfloat16), tp_count)
    others = []
    for k in range(1, tp_count):
        piece = lax.dynamic_index_in_dim(ordered, tp ^ k, axis=1, keepdims=False)
        others.append(lax.ppermute(piece, "tp", [(i, i ^ k) for i in range(tp_count)]))
    gathered = lax.all_gather(jnp.concatenate(others, axis=0), "dp", axis=0, tiled=True)
    out = place(None, own_gathered, tp, 0, 1, tp_count, rows)
    out = place(out, gathered, tp, 1, tp_count, tp_count, rows)
    return (new_master, new_avg, new_avg_sq, out)


def solution(mesh):
    rows = P(("dp", "tp"), None)
    return jax.shard_map(
        body, mesh=mesh, in_specs=(rows,) * 4, out_specs=(rows, rows, rows, P(None, "tp")), check_vma=False
    )
```
